32 devices in a mesh: depth: 8 (over z, x), col: 4 (over y, core).
Axes of the slice: x: 2, y: 2, z: 4, core: 2. Of those that a mesh axis runs over, the one named last changes fastest.
Arguments:
- recorded: bfloat16 [4, 16, 2, 512, 512], P(None, 'depth', None, 'col'), may hold values from -6 to 6
- vertical: float32 [4, 512], replicated, may hold values from 0.05 to 0.8
Outputs:
- prediction: float32 [4, 2, 512, 512], P(None, None, 'col', 'depth')
The draws below stay inside these ranges and needn't reach their ends.
All inputs are finite; a program needn't handle non-finite values.
Results may differ from the reference program's by a relative error of at most 0.01.
Values may be sent and summed in bfloat16 or wider, within the bound.
A program may use at most 64 MiB of HBM per device.

```python
import jax
import jax.numpy as jnp
from jax import lax

K = 512
W = 4
NZ = 16


def levels(stream_key, dims, pieces, least, high):
    factor_of, own = 1.0, jax.random.fold_in(stream_key, 6)
    for dim, blocks in pieces:
        steps = jnp.exp(jax.random.uniform(jax.random.fold_in(own, dim), (blocks,), jnp.float32, least / len(pieces), high / len(pieces)))
        factor_of = factor_of * jnp.repeat(steps, dims[dim] // blocks).reshape([-1 if axis == dim else 1 for axis in range(len(dims))])
    return factor_of


def gaussian(rng, extent, width, bound, shards=(), kind=jnp.bfloat16):
    drawn = jax.random.normal(rng, extent, jnp.float32) * width
    if len(shards) > 0:
        drawn = levels(rng, extent, shards, -0.22, 0.18) * drawn
    return jnp.clip(drawn, min=-bound, max=bound).astype(kind)


def setup_inputs(seed: int = 0) -> dict:
    keys = jax.random.split(jax.random.key(seed), 3)
    return {
        "recorded": gaussian(keys[0], (W, NZ, 2, K, K), 1.0, 6.0, ((1, 8), (3, 4))),
        "vertical": jnp.clip(jax.random.uniform(keys[1], (W, K), jnp.float32, 0.05, 0.8), 0.05, 0.8),
    }


def complex_product(left_side, right_side, pattern, stack_axis):
    left_real = left_side[:, :, 0].astype(jnp.float32)
    left_imag = left_side[:, :, 1].astype(jnp.float32)
    right_real = right_side[:, :, 0].astype(jnp.float32)
    right_imag = right_side[:, :, 1].astype(jnp.float32)
    real_part = jnp.einsum(pattern, left_real, right_real) - jnp.einsum(pattern, left_imag, right_imag)
    imag_part = jnp.einsum(pattern, left_real, right_imag) + jnp.einsum(pattern, left_imag, right_real)
    return jnp.stack([real_part, imag_part], axis=stack_axis)


def reference(recorded, vertical):
    depth_step = 1.0 / NZ
    depth_f = jnp.arange(NZ, dtype=jnp.int32).astype(jnp.float32)
    phase_angle = (vertical[:, None, :, None] + vertical[:, None, None, :]) * depth_f[None, :, None, None]
    cosine = jnp.cos(phase_angle)
    sine_part = jnp.sin(phase_angle)
    real_in = recorded[:, :, 0].astype(jnp.float32)
    imag_in = recorded[:, :, 1].astype(jnp.float32)
    plus32 = jnp.stack([real_in * cosine - imag_in * sine_part, real_in * sine_part + imag_in * cosine], axis=2) * depth_step
    minus_phase = (jnp.stack([real_in * cosine + imag_in * sine_part, imag_in * cosine - real_in * sine_part], axis=2) * depth_step).astype(jnp.bfloat16)
    plus_phase = plus32.astype(jnp.bfloat16)
    suffix_all = lax.cumsum(plus32, axis=1, reverse=True)
    tail_sum = jnp.concatenate([suffix_all[:, 1:], jnp.zeros_like(suffix_all[:, :1])], axis=1).astype(jnp.bfloat16)
    products = complex_product(minus_phase, tail_sum, "wzrk,wzkc->wzrc", 2)
    running = lax.cumsum(products, axis=1)
    lagged = jnp.concatenate([jnp.zeros_like(running[:, :1]), running[:, :-1]], axis=1).astype(jnp.bfloat16)
    return complex_product(plus_phase, lagged, "wzrk,wzkc->wrc", 1)
```

```python
import functools

import jax
import jax.numpy as jnp
from jax import lax
from jax.experimental import pallas as pl
from jax.experimental.pallas import tpu as pltpu
from jax.sharding import PartitionSpec as P

MESH = pl.DeviceIdType.MESH


def prefix(x, axis, combine, identity):
    peers, mine = (lax.axis_size(axis), lax.axis_index(axis))
    everything = lax.all_gather(x, axis)
    start = jnp.broadcast_to(jnp.asarray(identity, x.dtype), x.shape)

    def lap(k, before):
        at = peers - 1 - k
        reached = at > mine
        new = combine(before, everything[at])
        return jnp.where(reached, new, before)

    return lax.fori_loop(0, peers, lap, start)


def from_behind(value, axis, steps):
    count = lax.axis_size(axis)
    initial, last = (max(0, -steps), min(count, count - steps))
    return lax.ppermute(value, axis, [(source, source + steps) for source in range(initial, last)])


def complex_product(left_side, right_side, pattern, stack_axis):
    left_real = left_side[:, :, 0]
    left_imag = left_side[:, :, 1]
    right_real = right_side[:, :, 0]
    right_imag = right_side[:, :, 1]
    real_part = jnp.einsum(
        pattern, left_real, right_real, preferred_element_type=jnp.float32
    ) - jnp.einsum(pattern, left_imag, right_imag, preferred_element_type=jnp.float32)
    imag_part = jnp.einsum(
        pattern, left_real, right_imag, preferred_element_type=jnp.float32
    ) + jnp.einsum(pattern, left_imag, right_real, preferred_element_type=jnp.float32)
    return jnp.stack([real_part, imag_part], axis=stack_axis)


def add_pair(earlier, later):
    return earlier + later


def shards(recorded, vertical):
    local_depths = recorded.shape[1]
    row_count = recorded.shape[3]
    depth_cells = lax.axis_size("depth") * local_depths
    depth_step = 1.0 / depth_cells
    first_row = lax.axis_index("col") * row_count
    row_wave = lax.dynamic_slice_in_dim(vertical, first_row, row_count, 1)
    depth_f = (
        lax.axis_index("depth") * local_depths + jnp.arange(local_depths, dtype=jnp.int32)
    ).astype(jnp.float32)
    phase_angle = (row_wave[:, None, :, None] + vertical[:, None, None, :]) * depth_f[
        None, :, None, None
    ]
    cosine = jnp.cos(phase_angle)
    sine_part = jnp.sin(phase_angle)
    real_in = recorded[:, :, 0].astype(jnp.float32)
    imag_in = recorded[:, :, 1].astype(jnp.float32)
    plus32 = (
        jnp.stack(
            [real_in * cosine - imag_in * sine_part, real_in * sine_part + imag_in * cosine], axis=2
        )
        * depth_step
    )
    minus_phase = (
        jnp.stack(
            [real_in * cosine + imag_in * sine_part, imag_in * cosine - real_in * sine_part], axis=2
        )
        * depth_step
    ).astype(jnp.bfloat16)
    inner_sum = lax.cumsum(plus32, axis=1, reverse=True)
    beyond = prefix(inner_sum[:, 0], "depth", add_pair, jnp.zeros_like(inner_sum[:, 0]))
    suffix_all = inner_sum + beyond[:, None]
    following = from_behind(suffix_all[:, 0], "depth", -1)
    tail_sum = jnp.concatenate([suffix_all[:, 1:], following[:, None]], axis=1).astype(jnp.bfloat16)
    columns = tail_sum
    middle = complex_product(
        columns, lax.all_gather(minus_phase, "col", axis=3, tiled=True), "wzrk,wzkc->wzrc", 2
    ).astype(jnp.bfloat16)
    columns = middle
    partial_pred = complex_product(
        columns, lax.all_gather(tail_sum, "col", axis=3, tiled=True), "wzrk,wzkc->wrc", 1
    )
    return lax.psum_scatter(partial_pred, "depth", scatter_dimension=3, tiled=True)


def kernel(
    sizes, rec, ct, rt, out, land, ml, tl, ts, prod, suf, sbuf, srecv, ein, eout, xsend, xrecv,
    pacc, psend, precv, qsend, qrecv, qsum, fsend, frecv,
    a_send, a_recv, s_send, s_recv, e_send, e_recv, x_send, x_recv, p_send, p_recv,
    q_send, q_recv, f_send, f_recv,
):
    levels, freqs, cols, local, rows, size, width = sizes
    depth, col = lax.axis_index("depth"), lax.axis_index("col")
    z, x = depth // 2, depth % 2
    y, core = col // 2, col % 2
    rings = cols // 2
    half = size // 2
    chunks = size // width
    f32, bf16 = jnp.float32, jnp.bfloat16

    def device(zz, xx, yy, cc):
        return (zz * 2 + xx, yy * 2 + cc)

    other_core = device(z, x, y, 1 - core)
    barrier = pltpu.get_barrier_semaphore()
    greeted = 0
    for dx in range(2):
        for dc in range(cols):
            if dx or dc:
                pl.semaphore_signal(
                    barrier, inc=1,
                    device_id=(z * 2 + (x + dx) % 2, (col + dc) % cols), device_id_type=MESH,
                )
                greeted += 1
    for dz in range(1, levels):
        pl.semaphore_signal(
            barrier, inc=1, device_id=(((z + dz) % levels) * 2 + x, col), device_id_type=MESH
        )
        greeted += 1
    pl.semaphore_wait(barrier, greeted)

    def remote(src, dst, send, recv, to):
        return pltpu.make_async_remote_copy(
            src_ref=src, dst_ref=dst, send_sem=send, recv_sem=recv, device_id=to, device_id_type=MESH
        )

    def spread(j, dx, dy, near=False):
        xx, yy = (x + dx) % 2, (y + dy) % rings
        w = yy * 2 + xx
        src = rec.at[w, :, :, :, pl.ds(j * width, width)]
        dst = land.at[:, :, pl.ds(pl.multiple_of(col * rows, rows), rows), pl.ds(j * width, width)]
        if near:
            return pltpu.make_async_copy(src, dst, a_recv.at[j, col])
        return remote(src, dst, a_send.at[j, dy * 2 + dx], a_recv.at[j, col], device(z, xx, yy, x))

    routes = [(dx, dy) for dy in reversed(range(rings)) for dx in (1, 0)]
    for j in range(chunks):
        for dx, dy in routes:
            if dx or dy:
                spread(j, dx, dy).start()
            else:
                pl.when(core == x)(lambda: spread(j, dx, dy, near=True).start())
                pl.when(core != x)(lambda: spread(j, dx, dy).start())

    @pl.when(z == levels - 1)
    def _():
        ein[...] = jnp.zeros_like(ein)

    tile = 64

    def phase(j):
        for source in range(cols):
            dst = land.at[:, :, pl.ds(source * rows, rows), pl.ds(j * width, width)]
            pltpu.make_async_copy(dst, dst, a_recv.at[j, source]).wait()
        lanes = pl.ds(j * width, width)

        @pl.loop(0, size // tile)
        def _(t):
            start = pl.multiple_of(t * tile, tile)
            at = pl.ds(start, tile)
            low = pl.ds(start + size, tile)
            sum_re = sum_im = None
            for l in reversed(range(local)):
                if sum_re is not None:
                    suf[l, 0, at, lanes] = sum_re
                    suf[l, 1, at, lanes] = sum_im
                re = land[l, 0, at, lanes].astype(f32)
                im = land[l, 1, at, lanes].astype(f32)
                row_cos, row_sin = ct[at, 2 * l : 2 * l + 1], ct[at, 2 * l + 1 : 2 * l + 2]
                col_cos, col_sin = rt[2 * l : 2 * l + 1, lanes], rt[2 * l + 1 : 2 * l + 2, lanes]
                cosine = row_cos * col_cos - row_sin * col_sin
                sine = row_sin * col_cos + row_cos * col_sin
                a, b, c, d = re * cosine, im * sine, re * sine, im * cosine
                minus_re, minus_im = a + b, d - c
                shifted = pl.ds(size + j * width, width)
                ml[l, at, lanes] = minus_re.astype(bf16)
                ml[l, low, shifted] = minus_re.astype(bf16)
                ml[l, at, shifted] = (-minus_im).astype(bf16)
                ml[l, low, lanes] = minus_im.astype(bf16)
                plus_re, plus_im = a - b, c + d
                sum_re = plus_re if sum_re is None else sum_re + plus_re
                sum_im = plus_im if sum_im is None else sum_im + plus_im
            sbuf[j, 0, at, :] = sum_re.astype(bf16)
            sbuf[j, 1, at, :] = sum_im.astype(bf16)

        share(j).start()

    def share(j):
        theirs = pl.ds(pl.multiple_of((1 - core) * half, half), half)
        return remote(sbuf.at[j, :, theirs, :], srecv.at[j], s_send.at[j], s_recv.at[j], other_core)

    def down(j):
        to = device((z + levels - 1) % levels, x, y, core)
        return remote(eout.at[j], ein.at[j], e_send.at[j], e_recv.at[j], to)

    def across(j):
        return remote(xsend.at[j], xrecv.at[j], x_send.at[j], x_recv.at[j], other_core)

    def put_tail(j, start, deeper):
        at, low = pl.ds(start, tile), pl.ds(start + size, tile)
        lanes = pl.ds(j * width, width)
        for l in range(local):
            re, im = deeper
            if l < local - 1:
                re, im = re + suf[l, 0, at, lanes], im + suf[l, 1, at, lanes]
            base = 2 * size * l
            first = pl.ds(base + j * width, width)
            second = pl.ds(base + size + j * width, width)
            ts[l, at, lanes] = re.astype(bf16)
            ts[l, low, lanes] = im.astype(bf16)
            tl[at, first] = re.astype(bf16)
            tl[low, second] = re.astype(bf16)
            tl[at, second] = (-im).astype(bf16)
            tl[low, first] = im.astype(bf16)

    def chain(j):
        share(j).wait_recv()
        pl.when(z < levels - 1)(lambda: down(j).wait_recv())

        @pl.loop(0, half // tile)
        def _(t):
            start = pl.multiple_of(t * tile, tile)
            at = pl.ds(start, tile)
            mine = pl.ds(pl.multiple_of(core * half + start, tile), tile)
            for part in range(2):
                below = ein[j, part, at, :].astype(f32)
                own = sbuf[j, part, mine, :].astype(f32)
                their = srecv[j, part, at, :].astype(f32)
                eout[j, part, at, :] = (below + own + their).astype(bf16)
                xsend[j, part, at, :] = (below + jnp.where(core == 1, own, 0.0)).astype(bf16)

        pl.when(z > 0)(lambda: down(j).start())
        across(j).start()

        @pl.loop(0, half // tile)
        def _(t):
            start = pl.multiple_of(t * tile, tile)
            at = pl.ds(start, tile)
            deeper = [
                ein[j, part, at, :].astype(f32)
                + jnp.where(core == 0, srecv[j, part, at, :].astype(f32), 0.0)
                for part in range(2)
            ]
            put_tail(j, pl.multiple_of(core * half + start, tile), deeper)

    def finish(j):
        across(j).wait_recv()

        @pl.loop(0, half // tile)
        def _(t):
            start = pl.multiple_of(t * tile, tile)
            at = pl.ds(start, tile)
            deeper = [xrecv[j, part, at, :].astype(f32) for part in range(2)]
            put_tail(j, pl.multiple_of((1 - core) * half + start, tile), deeper)

    block = 2 * width
    blocks = size // block

    def middle(h):
        lanes = pl.ds(h * block, block)
        for l in range(local):
            @pl.loop(0, 2 * cols // 2)
            def _(t):
                at = pl.ds(pl.multiple_of(t * 2 * rows, 2 * rows), 2 * rows)
                low = pl.ds(pl.multiple_of(2 * size * l + t * 2 * rows, 2 * rows), 2 * rows)
                prod[low, lanes] = jnp.dot(
                    ml[l, at, :], ts[l, :, lanes], preferred_element_type=f32
                ).astype(bf16)

    for j in range(chunks):
        phase(j)
        chain(j)
        if j > 0:
            finish(j - 1)
    for h in range(blocks - 1):
        middle(h)
    finish(chunks - 1)
    middle(blocks - 1)

    tiles = 2 * rings
    order = [(z // 2 + 1 + i) % blocks for i in range(blocks)]

    def pair(i):
        return remote(psend.at[i], precv.at[i], p_send.at[i], p_recv.at[i], other_core)

    for i, h in enumerate(order):
        lanes = pl.ds(pl.multiple_of(h * block, block), block)

        @pl.loop(0, tiles)
        def _(t):
            at = pl.ds(pl.multiple_of(t * 2 * rows, 2 * rows), 2 * rows)
            pacc[i, t] = jnp.dot(tl[at, :], prod[:, lanes], preferred_element_type=f32)
            theirs = pl.ds(pl.multiple_of((1 - core) * rows, rows), rows)
            psend[i, t] = pacc[i, t, theirs, :].astype(bf16)

        pair(i).start()

    def to_level(target):
        return remote(
            qsend.at[target], qrecv.at[z], q_send.at[target], q_recv.at[z],
            device(target, x, y, core),
        )

    for i, h in enumerate(order):
        pair(i).wait_recv()
        for s in range(2):
            target = h * 2 + s
            lanes = pl.ds(s * width, width)

            @pl.loop(0, tiles)
            def _(t):
                mine = pl.ds(pl.multiple_of(core * rows, rows), rows)
                q = pacc[i, t, mine, lanes] + precv[i, t, :, lanes].astype(f32)
                qsend[target, t] = q.astype(bf16)

                @pl.when(target == z)
                def _():
                    qsum[t] = q

            pl.when(target != z)(lambda: to_level(target).start())

    for dz in range(1, levels):
        source = (z + dz) % levels
        remote(
            qsend.at[source], qrecv.at[source], q_send.at[source], q_recv.at[source],
            device(source, x, y, core),
        ).wait_recv()

        @pl.loop(0, tiles)
        def _(t):
            qsum[t] += qrecv[source, t].astype(f32)

    @pl.loop(0, tiles)
    def _(t):
        fsend[t % rings, t // rings] = qsum[t].astype(bf16)

    me = y * 2 + x

    def to_rows(dx, dy):
        xx, yy = (x + dx) % 2, (y + dy) % rings
        return remote(
            fsend.at[yy], frecv.at[me], f_send.at[dy * 2 + dx], f_recv.at[me],
            device(z, xx, yy, core),
        )

    narrow = width // 2

    def emit(w, part, value):
        out[w, part] = jnp.where(x == 0, value[:, :narrow], value[:, narrow:])

    for dx, dy in routes:
        if dx or dy:
            to_rows(dx, dy).start()
    for part in range(2):
        emit(me, part, qsum[part * rings + y])
    for dx, dy in reversed(routes):
        if dx or dy:
            xx, yy = (x + dx) % 2, (y + dy) % rings
            w = yy * 2 + xx
            remote(
                fsend.at[yy], frecv.at[w], f_send.at[dy * 2 + dx], f_recv.at[w],
                device(z, xx, yy, core),
            ).wait_recv()
            for part in range(2):
                emit(w, part, frecv[w, part].astype(f32))

    for j in range(chunks):
        for dx, dy in routes:
            if dx or dy:
                spread(j, dx, dy).wait_send()
            else:
                pl.when(core != x)(lambda: spread(j, dx, dy).wait_send())
        share(j).wait_send()
        pl.when(z > 0)(lambda: down(j).wait_send())
        across(j).wait_send()
    for i in range(blocks):
        pair(i).wait_send()
    for dz in range(1, levels):
        to_level((z + dz) % levels).wait_send()
    for dx, dy in routes:
        if dx or dy:
            to_rows(dx, dy).wait_send()


def fused(recorded, vertical):
    freqs, local, _, rows, size = recorded.shape
    depths, cols = lax.axis_size("depth"), lax.axis_size("col")
    levels, chunks_wide = depths // 2, 2 * size // depths
    depth, col = lax.axis_index("depth"), lax.axis_index("col")
    z, x, y, core = depth // 2, depth % 2, col // 2, col % 2
    wave = lax.dynamic_index_in_dim(vertical, y * 2 + x, 0, keepdims=False)
    index = ((z * 2 + core) * local + jnp.arange(local, dtype=jnp.int32)).astype(jnp.float32)
    angle = wave[None] * index[:, None]
    table = jnp.stack([jnp.cos(angle), jnp.sin(angle)], axis=1).reshape(2 * local, size)
    width = chunks_wide
    chunks, half, tiles, blocks = size // width, size // 2, cols, size // (2 * width)
    sizes = (levels, freqs, cols, local, rows, size, width)
    f32, bf16 = jnp.float32, jnp.bfloat16
    dma = pltpu.SemaphoreType.DMA
    return pl.pallas_call(
        functools.partial(kernel, sizes),
        out_shape=jax.ShapeDtypeStruct((freqs, 2, rows, size // depths), f32),
        in_specs=[
            pl.BlockSpec(memory_space=pl.ANY),
            pl.BlockSpec(memory_space=pltpu.VMEM),
            pl.BlockSpec(memory_space=pltpu.VMEM),
        ],
        out_specs=pl.BlockSpec(memory_space=pltpu.VMEM),
        scratch_shapes=[
            pltpu.VMEM((local, 2, size, size), bf16),
            pltpu.VMEM((local, 2 * size, 2 * size), bf16),
            pltpu.VMEM((2 * size, local * 2 * size), bf16),
            pltpu.VMEM((local, 2 * size, size), bf16),
            pltpu.VMEM((local * 2 * size, size), bf16),
            pltpu.VMEM((local - 1, 2, size, size), f32),
            pltpu.VMEM((chunks, 2, size, width), bf16),
            pltpu.VMEM((chunks, 2, half, width), bf16),
            pltpu.VMEM((chunks, 2, half, width), bf16),
            pltpu.VMEM((chunks, 2, half, width), bf16),
            pltpu.VMEM((chunks, 2, half, width), bf16),
            pltpu.VMEM((chunks, 2, half, width), bf16),
            pltpu.VMEM((blocks, tiles, 2 * rows, 2 * width), f32),
            pltpu.VMEM((blocks, tiles, rows, 2 * width), bf16),
            pltpu.VMEM((blocks, tiles, rows, 2 * width), bf16),
            pltpu.VMEM((levels, tiles, rows, width), bf16),
            pltpu.VMEM((levels, tiles, rows, width), bf16),
            pltpu.VMEM((tiles, rows, width), f32),
            pltpu.VMEM((cols // 2, 2, rows, width), bf16),
            pltpu.VMEM((freqs, 2, rows, width), bf16),
            dma((chunks, cols)), dma((chunks, cols)),
            dma((chunks,)), dma((chunks,)),
            dma((chunks,)), dma((chunks,)),
            dma((chunks,)), dma((chunks,)),
            dma((blocks,)), dma((blocks,)),
            dma((levels,)), dma((levels,)),
            dma((cols,)), dma((freqs,)),
        ],
        compiler_params=pltpu.CompilerParams(
            collective_id=0, has_side_effects=True, vmem_limit_bytes=56 * 1024 * 1024
        ),
        name="prediction",
    )(recorded, table.T, table * (1.0 / (depths * local)))


def body(recorded, vertical):
    freqs, local, _, rows, size = recorded.shape
    depths, cols = lax.axis_size("depth"), lax.axis_size("col")
    fits = cols == freqs and cols % 2 == 0 and depths % 4 == 0 and local > 1
    fits = fits and rows % 128 == 0 and (2 * size // depths) % 128 == 0
    return fused(recorded, vertical) if fits else shards(recorded, vertical)


def solution(mesh):
    in_specs = (P(None, "depth", None, "col", None), P())
    out_specs = P(None, None, "col", "depth")
    return jax.shard_map(body, mesh=mesh, in_specs=in_specs, out_specs=out_specs, check_vma=False)
```

```python
import functools

import jax
import jax.numpy as jnp
from jax import lax
from jax.experimental import pallas as pl
from jax.experimental.pallas import tpu as pltpu
from jax.sharding import PartitionSpec as P

MESH = pl.DeviceIdType.MESH
SPLITS = 2


def prefix(x, axis, combine, identity):
    peers, mine = (lax.axis_size(axis), lax.axis_index(axis))
    everything = lax.all_gather(x, axis)
    start = jnp.broadcast_to(jnp.asarray(identity, x.dtype), x.shape)

    def lap(k, before):
        at = peers - 1 - k
        reached = at > mine
        new = combine(before, everything[at])
        return jnp.where(reached, new, before)

    return lax.fori_loop(0, peers, lap, start)


def from_behind(value, axis, steps):
    count = lax.axis_size(axis)
    initial, last = (max(0, -steps), min(count, count - steps))
    return lax.ppermute(value, axis, [(source, source + steps) for source in range(initial, last)])


def complex_product(left_side, right_side, pattern, stack_axis):
    left_real = left_side[:, :, 0]
    left_imag = left_side[:, :, 1]
    right_real = right_side[:, :, 0]
    right_imag = right_side[:, :, 1]
    real_part = jnp.einsum(
        pattern, left_real, right_real, preferred_element_type=jnp.float32
    ) - jnp.einsum(pattern, left_imag, right_imag, preferred_element_type=jnp.float32)
    imag_part = jnp.einsum(
        pattern, left_real, right_imag, preferred_element_type=jnp.float32
    ) + jnp.einsum(pattern, left_imag, right_real, preferred_element_type=jnp.float32)
    return jnp.stack([real_part, imag_part], axis=stack_axis)


def add_pair(earlier, later):
    return earlier + later


def shards(recorded, vertical):
    local_depths = recorded.shape[1]
    row_count = recorded.shape[3]
    depth_cells = lax.axis_size("depth") * local_depths
    depth_step = 1.0 / depth_cells
    first_row = lax.axis_index("col") * row_count
    row_wave = lax.dynamic_slice_in_dim(vertical, first_row, row_count, 1)
    depth_f = (
        lax.axis_index("depth") * local_depths + jnp.arange(local_depths, dtype=jnp.int32)
    ).astype(jnp.float32)
    phase_angle = (row_wave[:, None, :, None] + vertical[:, None, None, :]) * depth_f[
        None, :, None, None
    ]
    cosine = jnp.cos(phase_angle)
    sine_part = jnp.sin(phase_angle)
    real_in = recorded[:, :, 0].astype(jnp.float32)
    imag_in = recorded[:, :, 1].astype(jnp.float32)
    plus32 = (
        jnp.stack(
            [real_in * cosine - imag_in * sine_part, real_in * sine_part + imag_in * cosine], axis=2
        )
        * depth_step
    )
    minus_phase = (
        jnp.stack(
            [real_in * cosine + imag_in * sine_part, imag_in * cosine - real_in * sine_part], axis=2
        )
        * depth_step
    ).astype(jnp.bfloat16)
    inner_sum = lax.cumsum(plus32, axis=1, reverse=True)
    beyond = prefix(inner_sum[:, 0], "depth", add_pair, jnp.zeros_like(inner_sum[:, 0]))
    suffix_all = inner_sum + beyond[:, None]
    following = from_behind(suffix_all[:, 0], "depth", -1)
    tail_sum = jnp.concatenate([suffix_all[:, 1:], following[:, None]], axis=1).astype(jnp.bfloat16)
    columns = tail_sum
    middle = complex_product(
        columns, lax.all_gather(minus_phase, "col", axis=3, tiled=True), "wzrk,wzkc->wzrc", 2
    ).astype(jnp.bfloat16)
    columns = middle
    partial_pred = complex_product(
        columns, lax.all_gather(tail_sum, "col", axis=3, tiled=True), "wzrk,wzkc->wrc", 1
    )
    return lax.psum_scatter(partial_pred, "depth", scatter_dimension=3, tiled=True)


def kernel(
    sizes, rec, vertical, out, waves, table, ct, rt, land, ml, tl, ts, prod, suf, sbuf, srecv, ein, eout, xsend, xrecv,
    pacc, psend, precv, qsend, qrecv, qsum, fsend, frecv,
    v_sem, a_send, a_recv, s_send, s_recv, e_send, e_recv, x_send, x_recv, p_send, p_recv,
    q_send, q_recv, f_send, f_recv,
):
    levels, freqs, cols, local, rows, size, width, splits = sizes
    depth, col = lax.axis_index("depth"), lax.axis_index("col")
    z, x = depth // 2, depth % 2
    y, core = col // 2, col % 2
    rings = cols // 2
    chunks = size // width
    sub = rows // splits
    share_rows = cols * sub // 2
    me = y * 2 + x
    f32, bf16 = jnp.float32, jnp.bfloat16

    def device(zz, xx, yy, cc):
        return (zz * 2 + xx, yy * 2 + cc)

    other_core = device(z, x, y, 1 - core)
    fetch = pltpu.make_async_copy(vertical, waves, v_sem)
    fetch.start()
    barrier = pltpu.get_barrier_semaphore()
    greeted = 0
    for dx in range(2):
        for dc in range(cols):
            if dx or dc:
                pl.semaphore_signal(
                    barrier, inc=1,
                    device_id=(z * 2 + (x + dx) % 2, (col + dc) % cols), device_id_type=MESH,
                )
                greeted += 1
    for dz in range(1, levels):
        pl.semaphore_signal(
            barrier, inc=1, device_id=(((z + dz) % levels) * 2 + x, col), device_id_type=MESH
        )
        greeted += 1
    pl.semaphore_wait(barrier, greeted)

    def remote(src, dst, send, recv, to):
        return pltpu.make_async_remote_copy(
            src_ref=src, dst_ref=dst, send_sem=send, recv_sem=recv, device_id=to, device_id_type=MESH
        )

    pieces = [(j, r) for j in range(chunks) for r in range(splits)]

    def spread(n, dx, dy, near=False):
        j, r = pieces[n]
        xx, yy = (x + dx) % 2, (y + dy) % rings
        w = yy * 2 + xx
        lanes = pl.ds(j * width, width)
        src = rec.at[w, :, :, pl.ds(r * sub, sub), lanes]
        dst = land.at[:, :, pl.ds(pl.multiple_of(col * rows + r * sub, sub), sub), lanes]
        if near:
            return pltpu.make_async_copy(src, dst, a_recv.at[n, col])
        return remote(src, dst, a_send.at[n, dy * 2 + dx], a_recv.at[n, col], device(z, xx, yy, x))

    routes = [(dx, dy) for dy in reversed(range(rings)) for dx in (1, 0)]
    for n in range(len(pieces)):
        for dx, dy in routes:
            if dx or dy:
                spread(n, dx, dy).start()
            else:
                pl.when(core == x)(lambda: spread(n, dx, dy, near=True).start())
                pl.when(core != x)(lambda: spread(n, dx, dy).start())

    @pl.when(z == levels - 1)
    def _():
        ein[...] = jnp.zeros_like(ein)

    fetch.wait()
    wave = waves[pl.ds(me, 1), :]
    table[...] = jnp.zeros_like(table)
    for l in range(local):
        angle = wave * ((z * 2 + core) * local + l).astype(f32)
        table[2 * l : 2 * l + 1, :] = jnp.cos(angle)
        table[2 * l + 1 : 2 * l + 2, :] = jnp.sin(angle)
    ct[...] = table[...].T
    rt[...] = table[0 : 2 * local, :] * (1.0 / (2 * levels * local))

    tile = sub

    def phase(n):
        j, r = pieces[n]
        for source in range(cols):
            dst = land.at[:, :, pl.ds(source * rows + r * sub, sub), pl.ds(j * width, width)]
            pltpu.make_async_copy(dst, dst, a_recv.at[n, source]).wait()
        lanes = pl.ds(j * width, width)

        @pl.loop(0, cols)
        def _(t):
            start = pl.multiple_of(t * rows + r * sub, sub)
            at = pl.ds(start, tile)
            low = pl.ds(start + size, tile)
            sum_re = sum_im = None
            for l in reversed(range(local)):
                if sum_re is not None:
                    suf[l, 0, at, lanes] = sum_re
                    suf[l, 1, at, lanes] = sum_im
                re = land[l, 0, at, lanes].astype(f32)
                im = land[l, 1, at, lanes].astype(f32)
                row_cos, row_sin = ct[at, 2 * l : 2 * l + 1], ct[at, 2 * l + 1 : 2 * l + 2]
                col_cos, col_sin = rt[2 * l : 2 * l + 1, lanes], rt[2 * l + 1 : 2 * l + 2, lanes]
                cosine = row_cos * col_cos - row_sin * col_sin
                sine = row_sin * col_cos + row_cos * col_sin
                a, b, c, d = re * cosine, im * sine, re * sine, im * cosine
                minus_re, minus_im = a + b, d - c
                shifted = pl.ds(size + j * width, width)
                ml[l, at, lanes] = minus_re.astype(bf16)
                ml[l, low, shifted] = minus_re.astype(bf16)
                ml[l, at, shifted] = (-minus_im).astype(bf16)
                ml[l, low, lanes] = minus_im.astype(bf16)
                plus_re, plus_im = a - b, c + d
                sum_re = plus_re if sum_re is None else sum_re + plus_re
                sum_im = plus_im if sum_im is None else sum_im + plus_im
            packed = pl.ds(pl.multiple_of(t * sub, sub), sub)
            sbuf[n, 0, packed, :] = sum_re.astype(bf16)
            sbuf[n, 1, packed, :] = sum_im.astype(bf16)

        share(n).start()

    def share(j):
        theirs = pl.ds(pl.multiple_of((1 - core) * share_rows, share_rows), share_rows)
        return remote(sbuf.at[j, :, theirs, :], srecv.at[j], s_send.at[j], s_recv.at[j], other_core)

    def down(j):
        to = device((z + levels - 1) % levels, x, y, core)
        return remote(eout.at[j], ein.at[j], e_send.at[j], e_recv.at[j], to)

    def across(j):
        return remote(xsend.at[j], xrecv.at[j], x_send.at[j], x_recv.at[j], other_core)

    def put_tail(n, start, deeper):
        j = pieces[n][0]
        at, low = pl.ds(start, tile), pl.ds(start + size, tile)
        lanes = pl.ds(j * width, width)
        for l in range(local):
            re, im = deeper
            if l < local - 1:
                re, im = re + suf[l, 0, at, lanes], im + suf[l, 1, at, lanes]
            base = 2 * size * l
            first = pl.ds(base + j * width, width)
            second = pl.ds(base + size + j * width, width)
            ts[l, at, lanes] = re.astype(bf16)
            ts[l, low, lanes] = im.astype(bf16)
            tl[at, first] = re.astype(bf16)
            tl[low, second] = re.astype(bf16)
            tl[at, second] = (-im).astype(bf16)
            tl[low, first] = im.astype(bf16)

    def chain(n):
        r = pieces[n][1]
        share(n).wait_recv()
        pl.when(z < levels - 1)(lambda: down(n).wait_recv())

        @pl.loop(0, cols // 2)
        def _(t):
            start = pl.multiple_of(t * sub, sub)
            at = pl.ds(start, sub)
            mine = pl.ds(pl.multiple_of(core * share_rows + start, sub), sub)
            for part in range(2):
                below = ein[n, part, at, :].astype(f32)
                own = sbuf[n, part, mine, :].astype(f32)
                their = srecv[n, part, at, :].astype(f32)
                eout[n, part, at, :] = (below + own + their).astype(bf16)
                xsend[n, part, at, :] = (below + jnp.where(core == 1, own, 0.0)).astype(bf16)

        pl.when(z > 0)(lambda: down(n).start())
        across(n).start()

        @pl.loop(0, cols // 2)
        def _(t):
            at = pl.ds(pl.multiple_of(t * sub, sub), sub)
            deeper = [
                ein[n, part, at, :].astype(f32)
                + jnp.where(core == 0, srecv[n, part, at, :].astype(f32), 0.0)
                for part in range(2)
            ]
            start = (core * (cols // 2) + t) * rows + r * sub
            put_tail(n, pl.multiple_of(start, sub), deeper)

    def finish(n):
        r = pieces[n][1]
        across(n).wait_recv()

        @pl.loop(0, cols // 2)
        def _(t):
            at = pl.ds(pl.multiple_of(t * sub, sub), sub)
            deeper = [xrecv[n, part, at, :].astype(f32) for part in range(2)]
            start = ((1 - core) * (cols // 2) + t) * rows + r * sub
            put_tail(n, pl.multiple_of(start, sub), deeper)

    block = 2 * width
    blocks = size // block

    def middle(h):
        lanes = pl.ds(h * block, block)
        for l in range(local):
            @pl.loop(0, 2 * cols // 2)
            def _(t):
                at = pl.ds(pl.multiple_of(t * 2 * rows, 2 * rows), 2 * rows)
                low = pl.ds(pl.multiple_of(2 * size * l + t * 2 * rows, 2 * rows), 2 * rows)
                prod[low, lanes] = jnp.dot(
                    ml[l, at, :], ts[l, :, lanes], preferred_element_type=f32
                ).astype(bf16)

    last = len(pieces) - 1

    def early():
        for h in range(blocks - 1):
            middle(h)

    for n in range(last):
        phase(n)
        chain(n)
        if n > 0:
            finish(n - 1)
    phase(last)
    finish(last - 1)
    pl.when(z < levels - 1)(early)
    chain(last)
    pl.when(z == levels - 1)(early)
    finish(last)
    middle(blocks - 1)

    tiles = 2 * rings
    order = [(z // 2 + 1 + i) % blocks for i in range(blocks)]

    def pair(i):
        return remote(psend.at[i], precv.at[i], p_send.at[i], p_recv.at[i], other_core)

    for i, h in enumerate(order):
        lanes = pl.ds(pl.multiple_of(h * block, block), block)

        @pl.loop(0, tiles)
        def _(t):
            at = pl.ds(pl.multiple_of(t * 2 * rows, 2 * rows), 2 * rows)
            pacc[i, t] = jnp.dot(tl[at, :], prod[:, lanes], preferred_element_type=f32)
            theirs = pl.ds(pl.multiple_of((1 - core) * rows, rows), rows)
            psend[i, t] = pacc[i, t, theirs, :].astype(bf16)

        pair(i).start()

    def to_level(target):
        return remote(
            qsend.at[target], qrecv.at[z], q_send.at[target], q_recv.at[z],
            device(target, x, y, core),
        )

    for i, h in enumerate(order):
        pair(i).wait_recv()
        for s in range(2):
            target = h * 2 + s
            lanes = pl.ds(s * width, width)

            @pl.loop(0, tiles)
            def _(t):
                mine = pl.ds(pl.multiple_of(core * rows, rows), rows)
                q = pacc[i, t, mine, lanes] + precv[i, t, :, lanes].astype(f32)
                qsend[target, t] = q.astype(bf16)

                @pl.when(target == z)
                def _():
                    qsum[t] = q

            pl.when(target != z)(lambda: to_level(target).start())

    for dz in range(1, levels):
        source = (z + dz) % levels
        remote(
            qsend.at[source], qrecv.at[source], q_send.at[source], q_recv.at[source],
            device(source, x, y, core),
        ).wait_recv()

        @pl.loop(0, tiles)
        def _(t):
            qsum[t] += qrecv[source, t].astype(f32)

    narrow = width // 2

    def joined(yy, xx):
        lanes = slice(xx * narrow, (xx + 1) * narrow)
        return jnp.concatenate([qsum[yy][:, lanes], qsum[rings + yy][:, lanes]], axis=1)

    for yy in range(rings):
        for xx in range(2):
            fsend[yy, xx] = joined(yy, xx).astype(bf16)

    def to_rows(dx, dy):
        xx, yy = (x + dx) % 2, (y + dy) % rings
        return remote(
            fsend.at[yy, xx], frecv.at[me], f_send.at[dy * 2 + dx], f_recv.at[me],
            device(z, xx, yy, core),
        )

    for dx, dy in routes:
        if dx or dy:
            to_rows(dx, dy).start()
    out[me] = jnp.where(x == 0, joined(y, 0), joined(y, 1))
    for dx, dy in reversed(routes):
        if dx or dy:
            xx, yy = (x + dx) % 2, (y + dy) % rings
            w = yy * 2 + xx
            remote(
                fsend.at[yy, xx], frecv.at[w], f_send.at[dy * 2 + dx], f_recv.at[w],
                device(z, xx, yy, core),
            ).wait_recv()
            out[w] = frecv[w].astype(f32)

    for n in range(len(pieces)):
        for dx, dy in routes:
            if dx or dy:
                spread(n, dx, dy).wait_send()
            else:
                pl.when(core != x)(lambda: spread(n, dx, dy).wait_send())
        share(n).wait_send()
        pl.when(z > 0)(lambda: down(n).wait_send())
        across(n).wait_send()
    for i in range(blocks):
        pair(i).wait_send()
    for dz in range(1, levels):
        to_level((z + dz) % levels).wait_send()
    for dx, dy in routes:
        if dx or dy:
            to_rows(dx, dy).wait_send()


def fused(recorded, vertical):
    freqs, local, _, rows, size = recorded.shape
    depths, cols = lax.axis_size("depth"), lax.axis_size("col")
    levels, chunks_wide = depths // 2, 2 * size // depths
    width = chunks_wide
    chunks, tiles, blocks = size // width, cols, size // (2 * width)
    pieces, share_rows = chunks * SPLITS, rows * cols // SPLITS // 2
    sizes = (levels, freqs, cols, local, rows, size, width, SPLITS)
    f32, bf16 = jnp.float32, jnp.bfloat16
    dma = pltpu.SemaphoreType.DMA
    packed = pl.pallas_call(
        functools.partial(kernel, sizes),
        out_shape=jax.ShapeDtypeStruct((freqs, rows, width), f32),
        in_specs=[
            pl.BlockSpec(memory_space=pl.ANY),
            pl.BlockSpec(memory_space=pl.ANY),
        ],
        out_specs=pl.BlockSpec(memory_space=pltpu.VMEM),
        scratch_shapes=[
            pltpu.VMEM((freqs, size), f32),
            pltpu.VMEM((128, size), f32),
            pltpu.VMEM((size, 128), f32),
            pltpu.VMEM((2 * local, size), f32),
            pltpu.VMEM((local, 2, size, size), bf16),
            pltpu.VMEM((local, 2 * size, 2 * size), bf16),
            pltpu.VMEM((2 * size, local * 2 * size), bf16),
            pltpu.VMEM((local, 2 * size, size), bf16),
            pltpu.VMEM((local * 2 * size, size), bf16),
            pltpu.VMEM((local - 1, 2, size, size), f32),
            pltpu.VMEM((pieces, 2, 2 * share_rows, width), bf16),
            pltpu.VMEM((pieces, 2, share_rows, width), bf16),
            pltpu.VMEM((pieces, 2, share_rows, width), bf16),
            pltpu.VMEM((pieces, 2, share_rows, width), bf16),
            pltpu.VMEM((pieces, 2, share_rows, width), bf16),
            pltpu.VMEM((pieces, 2, share_rows, width), bf16),
            pltpu.VMEM((blocks, tiles, 2 * rows, 2 * width), f32),
            pltpu.VMEM((blocks, tiles, rows, 2 * width), bf16),
            pltpu.VMEM((blocks, tiles, rows, 2 * width), bf16),
            pltpu.VMEM((levels, tiles, rows, width), bf16),
            pltpu.VMEM((levels, tiles, rows, width), bf16),
            pltpu.VMEM((tiles, rows, width), f32),
            pltpu.VMEM((cols // 2, 2, rows, width), bf16),
            pltpu.VMEM((freqs, rows, width), bf16),
            dma, dma((pieces, cols)), dma((pieces, cols)),
            dma((pieces,)), dma((pieces,)),
            dma((pieces,)), dma((pieces,)),
            dma((pieces,)), dma((pieces,)),
            dma((blocks,)), dma((blocks,)),
            dma((levels,)), dma((levels,)),
            dma((cols,)), dma((freqs,)),
        ],
        compiler_params=pltpu.CompilerParams(
            collective_id=0, has_side_effects=True, vmem_limit_bytes=56 * 1024 * 1024
        ),
        name="prediction",
    )(recorded, vertical)
    return jnp.stack([packed[:, :, : width // 2], packed[:, :, width // 2 :]], axis=1)


def body(recorded, vertical):
    freqs, local, _, rows, size = recorded.shape
    depths, cols = lax.axis_size("depth"), lax.axis_size("col")
    fits = cols == freqs and cols % 2 == 0 and depths % 4 == 0 and local > 1
    fits = fits and rows % 128 == 0 and (2 * size // depths) % 128 == 0
    return fused(recorded, vertical) if fits else shards(recorded, vertical)


def solution(mesh):
    in_specs = (P(None, "depth", None, "col", None), P())
    out_specs = P(None, None, "col", "depth")
    return jax.shard_map(body, mesh=mesh, in_specs=in_specs, out_specs=out_specs, check_vma=False)
```

```python
import functools

import jax
import jax.numpy as jnp
from jax import lax
from jax.experimental import pallas as pl
from jax.experimental.pallas import tpu as pltpu
from jax.sharding import PartitionSpec as P

MESH = pl.DeviceIdType.MESH
SPLITS = 4


def prefix(x, axis, combine, identity):
    peers, mine = (lax.axis_size(axis), lax.axis_index(axis))
    everything = lax.all_gather(x, axis)
    start = jnp.broadcast_to(jnp.asarray(identity, x.dtype), x.shape)

    def lap(k, before):
        at = peers - 1 - k
        reached = at > mine
        new = combine(before, everything[at])
        return jnp.where(reached, new, before)

    return lax.fori_loop(0, peers, lap, start)


def from_behind(value, axis, steps):
    count = lax.axis_size(axis)
    initial, last = (max(0, -steps), min(count, count - steps))
    return lax.ppermute(value, axis, [(source, source + steps) for source in range(initial, last)])


def complex_product(left_side, right_side, pattern, stack_axis):
    left_real = left_side[:, :, 0]
    left_imag = left_side[:, :, 1]
    right_real = right_side[:, :, 0]
    right_imag = right_side[:, :, 1]
    real_part = jnp.einsum(
        pattern, left_real, right_real, preferred_element_type=jnp.float32
    ) - jnp.einsum(pattern, left_imag, right_imag, preferred_element_type=jnp.float32)
    imag_part = jnp.einsum(
        pattern, left_real, right_imag, preferred_element_type=jnp.float32
    ) + jnp.einsum(pattern, left_imag, right_real, preferred_element_type=jnp.float32)
    return jnp.stack([real_part, imag_part], axis=stack_axis)


def add_pair(earlier, later):
    return earlier + later


def shards(recorded, vertical):
    local_depths = recorded.shape[1]
    row_count = recorded.shape[3]
    depth_cells = lax.axis_size("depth") * local_depths
    depth_step = 1.0 / depth_cells
    first_row = lax.axis_index("col") * row_count
    row_wave = lax.dynamic_slice_in_dim(vertical, first_row, row_count, 1)
    depth_f = (
        lax.axis_index("depth") * local_depths + jnp.arange(local_depths, dtype=jnp.int32)
    ).astype(jnp.float32)
    phase_angle = (row_wave[:, None, :, None] + vertical[:, None, None, :]) * depth_f[
        None, :, None, None
    ]
    cosine = jnp.cos(phase_angle)
    sine_part = jnp.sin(phase_angle)
    real_in = recorded[:, :, 0].astype(jnp.float32)
    imag_in = recorded[:, :, 1].astype(jnp.float32)
    plus32 = (
        jnp.stack(
            [real_in * cosine - imag_in * sine_part, real_in * sine_part + imag_in * cosine], axis=2
        )
        * depth_step
    )
    minus_phase = (
        jnp.stack(
            [real_in * cosine + imag_in * sine_part, imag_in * cosine - real_in * sine_part], axis=2
        )
        * depth_step
    ).astype(jnp.bfloat16)
    inner_sum = lax.cumsum(plus32, axis=1, reverse=True)
    beyond = prefix(inner_sum[:, 0], "depth", add_pair, jnp.zeros_like(inner_sum[:, 0]))
    suffix_all = inner_sum + beyond[:, None]
    following = from_behind(suffix_all[:, 0], "depth", -1)
    tail_sum = jnp.concatenate([suffix_all[:, 1:], following[:, None]], axis=1).astype(jnp.bfloat16)
    columns = tail_sum
    middle = complex_product(
        columns, lax.all_gather(minus_phase, "col", axis=3, tiled=True), "wzrk,wzkc->wzrc", 2
    ).astype(jnp.bfloat16)
    columns = middle
    partial_pred = complex_product(
        columns, lax.all_gather(tail_sum, "col", axis=3, tiled=True), "wzrk,wzkc->wrc", 1
    )
    return lax.psum_scatter(partial_pred, "depth", scatter_dimension=3, tiled=True)


def kernel(
    sizes, rec, vertical, out, waves, table, ct, rt, land, ml, tl, ts, prod, suf, sbuf, srecv, ein, eout, xsend, xrecv,
    pacc, psend, precv, qsend, qrecv, qsum, fsend, frecv,
    v_sem, a_send, a_recv, s_send, s_recv, e_send, e_recv, x_send, x_recv, p_send, p_recv,
    q_send, q_recv, f_send, f_recv,
):
    levels, freqs, cols, local, rows, size, width, splits = sizes
    depth, col = lax.axis_index("depth"), lax.axis_index("col")
    z, x = depth // 2, depth % 2
    y, core = col // 2, col % 2
    rings = cols // 2
    chunks = size // width
    sub = rows // splits
    share_rows = cols * sub // 2
    me = y * 2 + x
    f32, bf16 = jnp.float32, jnp.bfloat16

    def device(zz, xx, yy, cc):
        return (zz * 2 + xx, yy * 2 + cc)

    other_core = device(z, x, y, 1 - core)
    fetch = pltpu.make_async_copy(vertical, waves, v_sem)
    fetch.start()
    barrier = pltpu.get_barrier_semaphore()
    greeted = 0
    for dx in range(2):
        for dc in range(cols):
            if dx or dc:
                pl.semaphore_signal(
                    barrier, inc=1,
                    device_id=(z * 2 + (x + dx) % 2, (col + dc) % cols), device_id_type=MESH,
                )
                greeted += 1
    for dz in range(1, levels):
        pl.semaphore_signal(
            barrier, inc=1, device_id=(((z + dz) % levels) * 2 + x, col), device_id_type=MESH
        )
        greeted += 1
    pl.semaphore_wait(barrier, greeted)

    def remote(src, dst, send, recv, to):
        return pltpu.make_async_remote_copy(
            src_ref=src, dst_ref=dst, send_sem=send, recv_sem=recv, device_id=to, device_id_type=MESH
        )

    pieces = [(j, r) for j in range(chunks) for r in range(splits)]

    def spread(n, dx, dy, near=False):
        j, r = pieces[n]
        xx, yy = (x + dx) % 2, (y + dy) % rings
        w = yy * 2 + xx
        lanes = pl.ds(j * width, width)
        src = rec.at[w, :, :, pl.ds(r * sub, sub), lanes]
        dst = land.at[:, :, pl.ds(pl.multiple_of(col * rows + r * sub, sub), sub), lanes]
        if near:
            return pltpu.make_async_copy(src, dst, a_recv.at[n, col])
        return remote(src, dst, a_send.at[n, dy * 2 + dx], a_recv.at[n, col], device(z, xx, yy, x))

    routes = [(dx, dy) for dy in reversed(range(rings)) for dx in (1, 0)]
    for n in range(len(pieces)):
        for dx, dy in routes:
            if dx or dy:
                spread(n, dx, dy).start()
            else:
                pl.when(core == x)(lambda: spread(n, dx, dy, near=True).start())
                pl.when(core != x)(lambda: spread(n, dx, dy).start())

    @pl.when(z == levels - 1)
    def _():
        ein[...] = jnp.zeros_like(ein)

    fetch.wait()
    wave = waves[pl.ds(me, 1), :]
    table[...] = jnp.zeros_like(table)
    for l in range(local):
        angle = wave * ((z * 2 + core) * local + l).astype(f32)
        table[2 * l : 2 * l + 1, :] = jnp.cos(angle)
        table[2 * l + 1 : 2 * l + 2, :] = jnp.sin(angle)
    ct[...] = table[...].T
    rt[...] = table[0 : 2 * local, :] * (1.0 / (2 * levels * local))

    tile = sub

    def phase(n):
        j, r = pieces[n]
        for source in range(cols):
            dst = land.at[:, :, pl.ds(source * rows + r * sub, sub), pl.ds(j * width, width)]
            pltpu.make_async_copy(dst, dst, a_recv.at[n, source]).wait()
        lanes = pl.ds(j * width, width)

        @pl.loop(0, cols)
        def _(t):
            start = pl.multiple_of(t * rows + r * sub, sub)
            at = pl.ds(start, tile)
            low = pl.ds(start + size, tile)
            sum_re = sum_im = None
            for l in reversed(range(local)):
                if sum_re is not None:
                    suf[l, 0, at, lanes] = sum_re
                    suf[l, 1, at, lanes] = sum_im
                re = land[l, 0, at, lanes].astype(f32)
                im = land[l, 1, at, lanes].astype(f32)
                row_cos, row_sin = ct[at, 2 * l : 2 * l + 1], ct[at, 2 * l + 1 : 2 * l + 2]
                col_cos, col_sin = rt[2 * l : 2 * l + 1, lanes], rt[2 * l + 1 : 2 * l + 2, lanes]
                cosine = row_cos * col_cos - row_sin * col_sin
                sine = row_sin * col_cos + row_cos * col_sin
                a, b, c, d = re * cosine, im * sine, re * sine, im * cosine
                minus_re, minus_im = a + b, d - c
                shifted = pl.ds(size + j * width, width)
                ml[l, at, lanes] = minus_re.astype(bf16)
                ml[l, low, shifted] = minus_re.astype(bf16)
                ml[l, at, shifted] = (-minus_im).astype(bf16)
                ml[l, low, lanes] = minus_im.astype(bf16)
                plus_re, plus_im = a - b, c + d
                sum_re = plus_re if sum_re is None else sum_re + plus_re
                sum_im = plus_im if sum_im is None else sum_im + plus_im
            packed = pl.ds(pl.multiple_of(t * sub, sub), sub)
            sbuf[n, 0, packed, :] = sum_re.astype(bf16)
            sbuf[n, 1, packed, :] = sum_im.astype(bf16)

        share(n).start()

    def share(j):
        theirs = pl.ds(pl.multiple_of((1 - core) * share_rows, share_rows), share_rows)
        return remote(sbuf.at[j, :, theirs, :], srecv.at[j], s_send.at[j], s_recv.at[j], other_core)

    def down(j):
        to = device((z + levels - 1) % levels, x, y, core)
        return remote(eout.at[j], ein.at[j], e_send.at[j], e_recv.at[j], to)

    def across(j):
        return remote(xsend.at[j], xrecv.at[j], x_send.at[j], x_recv.at[j], other_core)

    def put_tail(n, start, deeper):
        j = pieces[n][0]
        at, low = pl.ds(start, tile), pl.ds(start + size, tile)
        lanes = pl.ds(j * width, width)
        for l in range(local):
            re, im = deeper
            if l < local - 1:
                re, im = re + suf[l, 0, at, lanes], im + suf[l, 1, at, lanes]
            base = 2 * size * l
            first = pl.ds(base + j * width, width)
            second = pl.ds(base + size + j * width, width)
            ts[l, at, lanes] = re.astype(bf16)
            ts[l, low, lanes] = im.astype(bf16)
            tl[at, first] = re.astype(bf16)
            tl[low, second] = re.astype(bf16)
            tl[at, second] = (-im).astype(bf16)
            tl[low, first] = im.astype(bf16)

    def chain(n):
        r = pieces[n][1]
        share(n).wait_recv()
        pl.when(z < levels - 1)(lambda: down(n).wait_recv())

        @pl.loop(0, cols // 2)
        def _(t):
            start = pl.multiple_of(t * sub, sub)
            at = pl.ds(start, sub)
            mine = pl.ds(pl.multiple_of(core * share_rows + start, sub), sub)
            for part in range(2):
                below = ein[n, part, at, :].astype(f32)
                own = sbuf[n, part, mine, :].astype(f32)
                their = srecv[n, part, at, :].astype(f32)
                eout[n, part, at, :] = (below + own + their).astype(bf16)
                xsend[n, part, at, :] = (below + jnp.where(core == 1, own, 0.0)).astype(bf16)

        pl.when(z > 0)(lambda: down(n).start())
        across(n).start()

        @pl.loop(0, cols // 2)
        def _(t):
            at = pl.ds(pl.multiple_of(t * sub, sub), sub)
            deeper = [
                ein[n, part, at, :].astype(f32)
                + jnp.where(core == 0, srecv[n, part, at, :].astype(f32), 0.0)
                for part in range(2)
            ]
            start = (core * (cols // 2) + t) * rows + r * sub
            put_tail(n, pl.multiple_of(start, sub), deeper)

    def finish(n):
        r = pieces[n][1]
        across(n).wait_recv()

        @pl.loop(0, cols // 2)
        def _(t):
            at = pl.ds(pl.multiple_of(t * sub, sub), sub)
            deeper = [xrecv[n, part, at, :].astype(f32) for part in range(2)]
            start = ((1 - core) * (cols // 2) + t) * rows + r * sub
            put_tail(n, pl.multiple_of(start, sub), deeper)

    block = 2 * width
    blocks = size // block

    def middle(h):
        lanes = pl.ds(h * block, block)
        for l in range(local):
            @pl.loop(0, 2 * cols // 2)
            def _(t):
                at = pl.ds(pl.multiple_of(t * 2 * rows, 2 * rows), 2 * rows)
                low = pl.ds(pl.multiple_of(2 * size * l + t * 2 * rows, 2 * rows), 2 * rows)
                prod[low, lanes] = jnp.dot(
                    ml[l, at, :], ts[l, :, lanes], preferred_element_type=f32
                ).astype(bf16)

    last = len(pieces) - 1

    def early():
        for h in range(blocks - 1):
            middle(h)

    for n in range(last):
        phase(n)
        chain(n)
        if n > 0:
            finish(n - 1)
    phase(last)
    finish(last - 1)
    pl.when(z < levels - 1)(early)
    chain(last)
    pl.when(z == levels - 1)(early)
    finish(last)
    middle(blocks - 1)

    tiles = 2 * rings
    order = [(z // 2 + 1 + i) % blocks for i in range(blocks)]

    def pair(i):
        return remote(psend.at[i], precv.at[i], p_send.at[i], p_recv.at[i], other_core)

    for i, h in enumerate(order):
        lanes = pl.ds(pl.multiple_of(h * block, block), block)

        @pl.loop(0, tiles)
        def _(t):
            at = pl.ds(pl.multiple_of(t * 2 * rows, 2 * rows), 2 * rows)
            pacc[i, t] = jnp.dot(tl[at, :], prod[:, lanes], preferred_element_type=f32)
            theirs = pl.ds(pl.multiple_of((1 - core) * rows, rows), rows)
            psend[i, t] = pacc[i, t, theirs, :].astype(bf16)

        pair(i).start()

    def to_level(target):
        return remote(
            qsend.at[target], qrecv.at[z], q_send.at[target], q_recv.at[z],
            device(target, x, y, core),
        )

    for i, h in enumerate(order):
        pair(i).wait_recv()
        for s in range(2):
            target = h * 2 + s
            lanes = pl.ds(s * width, width)

            @pl.loop(0, tiles)
            def _(t):
                mine = pl.ds(pl.multiple_of(core * rows, rows), rows)
                q = pacc[i, t, mine, lanes] + precv[i, t, :, lanes].astype(f32)
                qsend[target, t] = q.astype(bf16)

                @pl.when(target == z)
                def _():
                    qsum[t] = q

            pl.when(target != z)(lambda: to_level(target).start())

    for dz in range(1, levels):
        source = (z + dz) % levels
        remote(
            qsend.at[source], qrecv.at[source], q_send.at[source], q_recv.at[source],
            device(source, x, y, core),
        ).wait_recv()

        @pl.loop(0, tiles)
        def _(t):
            qsum[t] += qrecv[source, t].astype(f32)

    narrow = width // 2

    def joined(yy, xx):
        lanes = slice(xx * narrow, (xx + 1) * narrow)
        return jnp.concatenate([qsum[yy][:, lanes], qsum[rings + yy][:, lanes]], axis=1)

    for yy in range(rings):
        for xx in range(2):
            fsend[yy, xx] = joined(yy, xx).astype(bf16)

    def to_rows(dx, dy):
        xx, yy = (x + dx) % 2, (y + dy) % rings
        return remote(
            fsend.at[yy, xx], frecv.at[me], f_send.at[dy * 2 + dx], f_recv.at[me],
            device(z, xx, yy, core),
        )

    for dx, dy in routes:
        if dx or dy:
            to_rows(dx, dy).start()
    out[me] = jnp.where(x == 0, joined(y, 0), joined(y, 1))
    for dx, dy in reversed(routes):
        if dx or dy:
            xx, yy = (x + dx) % 2, (y + dy) % rings
            w = yy * 2 + xx
            remote(
                fsend.at[yy, xx], frecv.at[w], f_send.at[dy * 2 + dx], f_recv.at[w],
                device(z, xx, yy, core),
            ).wait_recv()
            out[w] = frecv[w].astype(f32)

    for n in range(len(pieces)):
        for dx, dy in routes:
            if dx or dy:
                spread(n, dx, dy).wait_send()
            else:
                pl.when(core != x)(lambda: spread(n, dx, dy).wait_send())
        share(n).wait_send()
        pl.when(z > 0)(lambda: down(n).wait_send())
        across(n).wait_send()
    for i in range(blocks):
        pair(i).wait_send()
    for dz in range(1, levels):
        to_level((z + dz) % levels).wait_send()
    for dx, dy in routes:
        if dx or dy:
            to_rows(dx, dy).wait_send()


def fused(recorded, vertical):
    freqs, local, _, rows, size = recorded.shape
    depths, cols = lax.axis_size("depth"), lax.axis_size("col")
    levels, chunks_wide = depths // 2, 2 * size // depths
    width = chunks_wide
    chunks, tiles, blocks = size // width, cols, size // (2 * width)
    pieces, share_rows = chunks * SPLITS, rows * cols // SPLITS // 2
    sizes = (levels, freqs, cols, local, rows, size, width, SPLITS)
    f32, bf16 = jnp.float32, jnp.bfloat16
    dma = pltpu.SemaphoreType.DMA
    packed = pl.pallas_call(
        functools.partial(kernel, sizes),
        out_shape=jax.ShapeDtypeStruct((freqs, rows, width), f32),
        in_specs=[
            pl.BlockSpec(memory_space=pl.ANY),
            pl.BlockSpec(memory_space=pl.ANY),
        ],
        out_specs=pl.BlockSpec(memory_space=pltpu.VMEM),
        scratch_shapes=[
            pltpu.VMEM((freqs, size), f32),
            pltpu.VMEM((128, size), f32),
            pltpu.VMEM((size, 128), f32),
            pltpu.VMEM((2 * local, size), f32),
            pltpu.VMEM((local, 2, size, size), bf16),
            pltpu.VMEM((local, 2 * size, 2 * size), bf16),
            pltpu.VMEM((2 * size, local * 2 * size), bf16),
            pltpu.VMEM((local, 2 * size, size), bf16),
            pltpu.VMEM((local * 2 * size, size), bf16),
            pltpu.VMEM((local - 1, 2, size, size), f32),
            pltpu.VMEM((pieces, 2, 2 * share_rows, width), bf16),
            pltpu.VMEM((pieces, 2, share_rows, width), bf16),
            pltpu.VMEM((pieces, 2, share_rows, width), bf16),
            pltpu.VMEM((pieces, 2, share_rows, width), bf16),
            pltpu.VMEM((pieces, 2, share_rows, width), bf16),
            pltpu.VMEM((pieces, 2, share_rows, width), bf16),
            pltpu.VMEM((blocks, tiles, 2 * rows, 2 * width), f32),
            pltpu.VMEM((blocks, tiles, rows, 2 * width), bf16),
            pltpu.VMEM((blocks, tiles, rows, 2 * width), bf16),
            pltpu.VMEM((levels, tiles, rows, width), bf16),
            pltpu.VMEM((levels, tiles, rows, width), bf16),
            pltpu.VMEM((tiles, rows, width), f32),
            pltpu.VMEM((cols // 2, 2, rows, width), bf16),
            pltpu.VMEM((freqs, rows, width), bf16),
            dma, dma((pieces, cols)), dma((pieces, cols)),
            dma((pieces,)), dma((pieces,)),
            dma((pieces,)), dma((pieces,)),
            dma((pieces,)), dma((pieces,)),
            dma((blocks,)), dma((blocks,)),
            dma((levels,)), dma((levels,)),
            dma((cols,)), dma((freqs,)),
        ],
        compiler_params=pltpu.CompilerParams(
            collective_id=0, has_side_effects=True, vmem_limit_bytes=56 * 1024 * 1024
        ),
        name="prediction",
    )(recorded, vertical)
    return packed.reshape(freqs, rows, 2, width // 2).transpose(0, 2, 1, 3)


def body(recorded, vertical):
    freqs, local, _, rows, size = recorded.shape
    depths, cols = lax.axis_size("depth"), lax.axis_size("col")
    fits = cols == freqs and cols % 2 == 0 and depths % 4 == 0 and local > 1
    fits = fits and rows % 128 == 0 and (2 * size // depths) % 128 == 0
    return fused(recorded, vertical) if fits else shards(recorded, vertical)


def solution(mesh):
    in_specs = (P(None, "depth", None, "col", None), P())
    out_specs = P(None, None, "col", "depth")
    return jax.shard_map(body, mesh=mesh, in_specs=in_specs, out_specs=out_specs, check_vma=False)
```
